32 devices in a mesh: amp: 32 (over z, y, x, core).
Axes of the slice: x: 2, y: 2, z: 4, core: 2. Of those that a mesh axis runs over, the one named last changes fastest.
Arguments:
- ket_state: float32 [2, 1048576], P(None, 'amp'), may hold values from -6 to 6
- observable: float32 [1048576], P('amp'), may hold values from -6 to 6
- angles: float32 [2, 3], replicated, may hold values from -3.140625 to 3.140625
- gate_kinds: int32 [2, 32], replicated, may hold values from 0 to 2
Outputs:
- bra_state: float32 [2, 1048576], P(None, 'amp')
- grads: float32 [2, 3], replicated
The draws below stay inside these ranges and needn't reach their ends.
Inputs may be any that keep to these rules, and one draw needn't show every extreme that they name: `gate_kinds`: 0 and 1 name rotations about Y with angles[l, 0] and angles[l, 1], 2 a rotation about Z with angles[l, 2]; entries for qubits at or above the number of qubits are not used.
All inputs are finite; a program needn't handle non-finite values.
Results may differ from the reference program's by a relative error of at most 0.0003.
Values sent between devices are 32-bit elements; how exact they have to be, the bound alone decides.
A program may use at most 128 MiB of HBM per device.

```python
import math
import jax
import jax.numpy as jnp
from jax import lax

AMPS_DEV = 32768
LAYERS = 2
KINDS = 3
QSLOTS = 32
AMPS = 1048576
N_AMP = 32


def set_ends(drawn, own_key, smallest, largest):
    shape = drawn.shape
    place = [jax.random.randint(jax.random.fold_in(own_key, axis), (), 0, shape[axis]) for axis in range(len(shape))]
    drawn = drawn.at[tuple(place)].set(smallest)
    longest = shape.index(max(shape))
    place[longest] = (place[longest] + 1) % shape[longest]
    return drawn.at[tuple(place)].set(largest)


def block_levels(rng, dims, pieces, low, largest):
    def one(position, blocks):
        draws = jax.random.uniform(jax.random.fold_in(jax.random.fold_in(rng, 6), position), (blocks,), jnp.float32, low / len(pieces), largest / len(pieces))
        return jnp.repeat(jnp.exp(draws), dims[position] // blocks).reshape((-1,) + (1,) * (len(dims) - position - 1))

    factor_of = one(*pieces[0])
    for cut in pieces[1:]:
        factor_of = factor_of * one(*cut)
    return factor_of


def normal_values(stream_key, dims, spread, limit, cuts=(), kind=jnp.bfloat16):
    drawn = spread * jax.random.normal(stream_key, dims, jnp.float32)
    if cuts:
        drawn = drawn * block_levels(stream_key, dims, cuts, -0.22, 0.18)
    return jnp.clip(drawn, -limit, limit).astype(kind)


def setup_inputs(seed: int = 0) -> dict:
    streams_of = jax.random.split(jax.random.key(seed), 5)
    return {
        "ket_state": normal_values(streams_of[0], (2, AMPS), 1.0, 6.0, ((1, 32),), jnp.float32),
        "observable": normal_values(streams_of[1], (AMPS,), 1.0, 6.0, ((0, 32),), jnp.float32),
        "angles": jnp.clip(jax.random.uniform(streams_of[2], (LAYERS, KINDS), jnp.float32, -3.140625, 3.140625), -3.140625, 3.140625),
        "gate_kinds": set_ends(jax.random.randint(streams_of[3], (LAYERS, QSLOTS), 0, 3), jax.random.fold_in(streams_of[3], 1), 0, 2).astype(jnp.int32),
    }


def rotate_phase(values, cosine, sine_value):
    return jnp.stack([cosine * values[0] - sine_value * values[1], cosine * values[1] + sine_value * values[0]])

def undo_qubit(ket_state, bra_state, qubit_id, rotation, is_z):
    amp_total = ket_state.shape[1]
    fold_shape = (2, amp_total >> qubit_id + 1, 2, 1 << qubit_id)
    cosine = jnp.cos(0.5 * rotation)
    sine_value = jnp.sin(0.5 * rotation)

    def turn_y(operands):
        folded_ket, folded_bra = operands
        ket_low, ket_high = (folded_ket[:, :, 0], folded_ket[:, :, 1])
        bra_low, bra_high = (folded_bra[:, :, 0], folded_bra[:, :, 1])
        partial_value = 0.5 * jnp.sum(bra_high * ket_low - bra_low * ket_high)
        new_ket = jnp.stack([cosine * ket_low + sine_value * ket_high, cosine * ket_high - sine_value * ket_low], axis=2)
        new_bra = jnp.stack([cosine * bra_low + sine_value * bra_high, cosine * bra_high - sine_value * bra_low], axis=2)
        return (new_ket, new_bra, partial_value)

    def turn_z(operands):
        folded_ket, folded_bra = operands
        ket_low, ket_high = (folded_ket[:, :, 0], folded_ket[:, :, 1])
        bra_low, bra_high = (folded_bra[:, :, 0], folded_bra[:, :, 1])
        partial_value = 0.5 * (jnp.sum(bra_low[0] * ket_low[1] - bra_low[1] * ket_low[0]) - jnp.sum(bra_high[0] * ket_high[1] - bra_high[1] * ket_high[0]))
        new_ket = jnp.stack([rotate_phase(ket_low, cosine, sine_value), rotate_phase(ket_high, cosine, -sine_value)], axis=2)
        new_bra = jnp.stack([rotate_phase(bra_low, cosine, sine_value), rotate_phase(bra_high, cosine, -sine_value)], axis=2)
        return (new_ket, new_bra, partial_value)
    new_ket, new_bra, partial_value = lax.cond(is_z, turn_z, turn_y, (ket_state.reshape(fold_shape), bra_state.reshape(fold_shape)))
    return (new_ket.reshape(2, amp_total), new_bra.reshape(2, amp_total), partial_value)

def reference(ket_state, observable, angles, gate_kinds):
    amp_total = AMPS_DEV * N_AMP
    all_bits = int(amp_total).bit_length() - 1
    bra_state = 2.0 / math.sqrt(amp_total) * observable[None, :] * ket_state
    amp_index = jnp.arange(amp_total, dtype=jnp.int32)
    parity = jnp.zeros((amp_total,), jnp.int32)
    for qubit_id in range(all_bits):
        neighbor = (qubit_id + 1) % all_bits
        parity = parity + (amp_index >> qubit_id & 1) * (amp_index >> neighbor & 1)
    phase_sign = (1 - 2 * (parity & 1)).astype(jnp.float32)
    grads = jnp.zeros((LAYERS, KINDS), jnp.float32)
    kind_range = jnp.arange(KINDS)
    layer_range = jnp.arange(LAYERS)
    for layer_id in reversed(range(LAYERS)):
        ket_state = ket_state * phase_sign[None, :]
        bra_state = bra_state * phase_sign[None, :]
        for qubit_id in range(all_bits):
            kind_id = gate_kinds[layer_id, qubit_id]
            rotation = jnp.sum(jnp.where(kind_range == kind_id, angles[layer_id], 0.0))
            ket_state, bra_state, partial_value = undo_qubit(ket_state, bra_state, qubit_id, rotation, kind_id == 2)
            selector = ((layer_range[:, None] == layer_id) & (kind_range[None, :] == kind_id)).astype(grads.dtype)
            grads = grads + partial_value * selector
    return (bra_state, grads)
```

```python
import functools
import math

import jax
import jax.numpy as jnp
import numpy as np
from jax import lax
from jax.experimental import pallas as pl
from jax.experimental.pallas import tpu as pltpu
from jax.sharding import PartitionSpec as P

MESH = pl.DeviceIdType.MESH
LANE, SUB, MAJOR, DEVICE = range(4)
LANE_BITS, SUB_BITS = 7, 3


def from_partner(value, axis, apart):
    mask = 2**apart
    pairs = [(source, source ^ mask) for source in range(lax.axis_size(axis))]
    return lax.ppermute(value, axis, pairs)


def pair_tables():
    column = np.arange(128)
    flips = []
    signs = []
    for position in range(7):
        upper = column >> position & 1
        flip_table = np.zeros((128, 128), np.float32)
        flip_table[column, column ^ 1 << position] = np.where(upper == 0, -0.5, 0.5)
        flips.append(flip_table)
        signs.append((1 - 2 * upper).astype(np.float32))
    return (np.stack(flips), np.stack(signs))


def layout_map(local_bits, global_bits):
    local_map = list(range(local_bits))
    device_map = [local_bits + bit_num for bit_num in range(global_bits)]
    return (local_map, device_map)


def entangle_sign(local_bits, global_bits, device_id, amp_count):
    local_map, device_map = layout_map(local_bits, global_bits)
    amp_index = lax.iota(jnp.int32, amp_count)
    bit_values = [None] * (local_bits + global_bits)
    for position in range(local_bits):
        bit_values[local_map[position]] = amp_index >> position & 1
    for bit_num in range(global_bits):
        bit_values[device_map[bit_num]] = device_id >> bit_num & 1
    all_bits = local_bits + global_bits
    parity = jnp.zeros((amp_count,), jnp.int32)
    for qubit_id in range(all_bits):
        parity = parity + bit_values[qubit_id] * bit_values[(qubit_id + 1) % all_bits]
    return (1 - 2 * (parity & 1)).astype(jnp.float32)


def rotation_of(angles, gate_kinds, layer_id, qubit_id):
    kind_id = gate_kinds[layer_id, qubit_id]
    chosen = jnp.arange(angles.shape[1]) == kind_id
    rotation = jnp.sum(jnp.where(chosen, angles[layer_id], 0.0))
    return (kind_id, jnp.cos(0.5 * rotation), jnp.sin(0.5 * rotation))


def kind_vector(kind_id, kind_count):
    return (jnp.arange(kind_count) == kind_id).astype(jnp.float32)


def rotate_phase(values, cosine, sine_value):
    return jnp.stack(
        [cosine * values[0] - sine_value * values[1], cosine * values[1] + sine_value * values[0]]
    )


def rotate_position(ket_state, bra_state, position, qubit_id, layer_id, angles, gate_kinds):
    amp_count = ket_state.shape[1]
    fold_shape = (2, amp_count >> position + 1, 2, 1 << position)
    kind_id, cosine, sine_value = rotation_of(angles, gate_kinds, layer_id, qubit_id)

    def turn_y(operands):
        folded_ket, folded_bra = operands
        ket_low, ket_high = (folded_ket[:, :, 0], folded_ket[:, :, 1])
        bra_low, bra_high = (folded_bra[:, :, 0], folded_bra[:, :, 1])
        partial_value = 0.5 * jnp.sum(bra_high * ket_low - bra_low * ket_high)
        new_ket = jnp.stack(
            [cosine * ket_low + sine_value * ket_high, cosine * ket_high - sine_value * ket_low],
            axis=2,
        )
        new_bra = jnp.stack(
            [cosine * bra_low + sine_value * bra_high, cosine * bra_high - sine_value * bra_low],
            axis=2,
        )
        return (new_ket, new_bra, partial_value)

    def turn_z(operands):
        folded_ket, folded_bra = operands
        ket_low, ket_high = (folded_ket[:, :, 0], folded_ket[:, :, 1])
        bra_low, bra_high = (folded_bra[:, :, 0], folded_bra[:, :, 1])
        partial_value = 0.5 * (
            jnp.sum(bra_low[0] * ket_low[1] - bra_low[1] * ket_low[0])
            - jnp.sum(bra_high[0] * ket_high[1] - bra_high[1] * ket_high[0])
        )
        new_ket = jnp.stack(
            [
                rotate_phase(ket_low, cosine, sine_value),
                rotate_phase(ket_high, cosine, -sine_value),
            ],
            axis=2,
        )
        new_bra = jnp.stack(
            [
                rotate_phase(bra_low, cosine, sine_value),
                rotate_phase(bra_high, cosine, -sine_value),
            ],
            axis=2,
        )
        return (new_ket, new_bra, partial_value)

    new_ket, new_bra, partial_value = lax.cond(
        kind_id == 2, turn_z, turn_y, (ket_state.reshape(fold_shape), bra_state.reshape(fold_shape))
    )
    terms = partial_value * kind_vector(kind_id, angles.shape[1])
    return (new_ket.reshape(2, amp_count), new_bra.reshape(2, amp_count), terms)


def contract_rows(left, right):
    return lax.dot_general(
        left,
        right,
        (((0,), (0,)), ((), ())),
        precision=lax.Precision.HIGHEST,
        preferred_element_type=jnp.float32,
    )


def contract_cols(left, right):
    return lax.dot_general(
        left,
        right,
        (((1,), (1,)), ((), ())),
        precision=lax.Precision.HIGHEST,
        preferred_element_type=jnp.float32,
    )


def low_block(ket_state, bra_state, qubit_list, layer_id, angles, gate_kinds):
    amp_count = ket_state.shape[1]
    row_count = amp_count // 128
    flips, signs = pair_tables()
    ket_real = ket_state[0].reshape(row_count, 128)
    ket_imag = ket_state[1].reshape(row_count, 128)
    bra_real = bra_state[0].reshape(row_count, 128)
    bra_imag = bra_state[1].reshape(row_count, 128)
    gram_real = contract_rows(bra_real, ket_real) + contract_rows(bra_imag, ket_imag)
    gram_imag = contract_rows(bra_real, ket_imag) - contract_rows(bra_imag, ket_real)
    gram_diag = jnp.diagonal(gram_imag)
    terms = jnp.zeros((angles.shape[1],), jnp.float32)
    kron_real = None
    kron_imag = None
    for position in range(7):
        kind_id, cosine, sine_value = rotation_of(
            angles, gate_kinds, layer_id, qubit_list[position]
        )
        is_z = kind_id == 2
        partial_value = jnp.where(
            is_z, 0.5 * jnp.sum(signs[position] * gram_diag), jnp.sum(flips[position] * gram_real)
        )
        terms = terms + partial_value * kind_vector(kind_id, angles.shape[1])
        mat_y = jnp.stack([jnp.stack([cosine, sine_value]), jnp.stack([-sine_value, cosine])])
        zero_value = jnp.zeros_like(cosine)
        mat_zr = jnp.stack([jnp.stack([cosine, zero_value]), jnp.stack([zero_value, cosine])])
        mat_zi = jnp.stack(
            [jnp.stack([sine_value, zero_value]), jnp.stack([zero_value, -sine_value])]
        )
        mat_real = jnp.where(is_z, mat_zr, mat_y)
        mat_imag = jnp.where(is_z, mat_zi, jnp.zeros_like(mat_zi))
        if kron_real is None:
            kron_real, kron_imag = (mat_real, mat_imag)
        else:
            kron_real, kron_imag = (
                jnp.kron(mat_real, kron_real) - jnp.kron(mat_imag, kron_imag),
                jnp.kron(mat_real, kron_imag) + jnp.kron(mat_imag, kron_real),
            )

    def apply_block(real_rows, imag_rows):
        new_real = contract_cols(real_rows, kron_real) - contract_cols(imag_rows, kron_imag)
        new_imag = contract_cols(imag_rows, kron_real) + contract_cols(real_rows, kron_imag)
        return jnp.stack([new_real.reshape(amp_count), new_imag.reshape(amp_count)])

    return (apply_block(ket_real, ket_imag), apply_block(bra_real, bra_imag), terms)


def rotate_global(
    ket_state,
    bra_state,
    far_ket,
    far_bra,
    bit_num,
    qubit_id,
    device_id,
    layer_id,
    angles,
    gate_kinds,
):
    kind_id, cosine, sine_value = rotation_of(angles, gate_kinds, layer_id, qubit_id)
    orient = (1 - 2 * (device_id >> bit_num & 1)).astype(jnp.float32)

    def turn_y(operands):
        own_ket, own_bra, other_ket, other_bra = operands
        partial_value = 0.25 * orient * jnp.sum(other_bra * own_ket - own_bra * other_ket)
        return (
            cosine * own_ket + orient * sine_value * other_ket,
            cosine * own_bra + orient * sine_value * other_bra,
            partial_value,
        )

    def turn_z(operands):
        own_ket, own_bra, other_ket, other_bra = operands
        partial_value = 0.5 * orient * jnp.sum(own_bra[0] * own_ket[1] - own_bra[1] * own_ket[0])
        return (
            rotate_phase(own_ket, cosine, orient * sine_value),
            rotate_phase(own_bra, cosine, orient * sine_value),
            partial_value,
        )

    new_ket, new_bra, partial_value = lax.cond(
        kind_id == 2, turn_z, turn_y, (ket_state, bra_state, far_ket, far_bra)
    )
    return (new_ket, new_bra, partial_value * kind_vector(kind_id, angles.shape[1]))


def on_device(ket_state, observable, angles, gate_kinds):
    amp_count = ket_state.shape[1]
    local_bits = amp_count.bit_length() - 1
    group_size = lax.axis_size("amp")
    global_bits = group_size.bit_length() - 1
    device_id = lax.axis_index("amp")
    layer_count = angles.shape[0]
    kind_count = angles.shape[1]
    bra_state = 2.0 / math.sqrt(amp_count * group_size) * observable[None, :] * ket_state
    sign_cache = {}
    grads_local = jnp.zeros((layer_count, kind_count), jnp.float32)
    for sweep_id in range(layer_count):
        layer_id = layer_count - 1 - sweep_id
        layout = 0
        local_map, device_map = layout_map(local_bits, global_bits)
        if layout not in sign_cache:
            sign_cache[layout] = entangle_sign(local_bits, global_bits, device_id, amp_count)
        phase_sign = sign_cache[layout]
        ket_state = ket_state * phase_sign[None, :]
        bra_state = bra_state * phase_sign[None, :]
        ket_state, bra_state, layer_terms = low_block(
            ket_state, bra_state, local_map[:7], layer_id, angles, gate_kinds
        )
        for position in range(7, local_bits):
            ket_state, bra_state, partial_value = rotate_position(
                ket_state, bra_state, position, local_map[position], layer_id, angles, gate_kinds
            )
            layer_terms = layer_terms + partial_value
        for bit_num in range(global_bits):
            far_ket, far_bra = from_partner((ket_state, bra_state), "amp", bit_num)
            ket_state, bra_state, partial_value = rotate_global(
                ket_state,
                bra_state,
                far_ket,
                far_bra,
                bit_num,
                device_map[bit_num],
                device_id,
                layer_id,
                angles,
                gate_kinds,
            )
            layer_terms = layer_terms + partial_value
        grads_local = grads_local.at[layer_id].set(layer_terms)
    grads = lax.psum(grads_local, "amp")
    return (bra_state, grads)


def layouts(major_bits, global_bits):
    low = LANE_BITS + SUB_BITS
    local_bits = low + major_bits
    home, away = {}, {}
    for q in range(LANE_BITS):
        home[q] = away[q] = (LANE, q)
    home[LANE_BITS] = away[LANE_BITS] = (SUB, 0)
    for bit, q in ((1, local_bits - 2), (2, local_bits - 1)):
        home[q] = away[q] = (SUB, bit)
    moved = list(range(low, local_bits - 2)) + [low - 2, low - 1]
    for bit, q in enumerate(moved):
        home[q], away[q] = (MAJOR, bit), (DEVICE, bit)
    for bit in range(global_bits):
        home[local_bits + bit], away[local_bits + bit] = (DEVICE, bit), (MAJOR, bit)
    return home, away


def split_major(x, bit):
    fold = x.reshape((x.shape[0] >> bit + 1, 2, 1 << bit) + x.shape[1:])
    return fold[:, 0], fold[:, 1]


def join_major(x0, x1):
    out = jnp.stack([x0, x1], axis=1)
    return out.reshape((-1,) + out.shape[3:])


def minor_bit(axis, bit):
    return lax.broadcasted_iota(jnp.int32, (1, 8, 128), 1 if axis == SUB else 2) >> bit & 1


def minor_sign(axis, bit):
    return (1 - 2 * minor_bit(axis, bit)).astype(jnp.float32)


def shifted(x, axis, by):
    dim = 1 if axis == SUB else 2
    return pltpu.roll(x, by % x.shape[dim], dim)


def partner(x, axis, bit):
    step = 1 << bit
    up = shifted(x, axis, -step)
    if 2 * step == x.shape[1 if axis == SUB else 2]:
        return up
    return jnp.where(minor_bit(axis, bit) == 0, up, shifted(x, axis, step))


def swap_bits(x, major, sub):
    x0, x1 = split_major(x, major)
    lower = minor_bit(SUB, sub) == 0

    def roll3(y, by):
        z = y.reshape((-1,) + y.shape[2:])
        return shifted(z, SUB, by).reshape(y.shape)

    step = 1 << sub
    return join_major(jnp.where(lower, x0, roll3(x1, step)), jnp.where(lower, roll3(x0, -step), x1))


def gate(state, place, coef):
    re, im = state
    axis, bit = place
    c, sy, sz = coef
    if axis == MAJOR:
        r0, r1 = split_major(re, bit)
        i0, i1 = split_major(im, bit)
        return (
            join_major(c * r0 + sy * r1 - sz * i0, c * r1 - sy * r0 + sz * i1),
            join_major(c * i0 + sy * i1 + sz * r0, c * i1 - sy * i0 - sz * r1),
        )
    z = minor_sign(axis, bit)
    zy, zz = sy * z, sz * z
    return (
        c * re + zy * partner(re, axis, bit) - zz * im,
        c * im + zy * partner(im, axis, bit) + zz * re,
    )


def terms(bra, ket, place, w, w_sum):
    axis, bit = place
    if axis == MAJOR:
        y = 0.0
        for b, k in zip(bra, ket):
            b0, b1 = split_major(b, bit)
            k0, k1 = split_major(k, bit)
            y = y + jnp.sum(b1 * k0 - b0 * k1, axis=(0, 1))
        w0, w1 = split_major(w, bit)
        return 0.5 * y, 0.5 * jnp.sum(w0 - w1, axis=(0, 1))
    z = 0.5 * minor_sign(axis, bit)[0]
    y = sum(jnp.sum(b * partner(k, axis, bit), axis=0) for b, k in zip(bra, ket))
    return -z * y, z * w_sum


def edge_sign(place, qubits, edges, majors, me):
    shape = (majors, 8, 128)
    parts = {
        LANE: lax.broadcasted_iota(jnp.int32, shape, 2),
        SUB: lax.broadcasted_iota(jnp.int32, shape, 1),
        MAJOR: lax.broadcasted_iota(jnp.int32, shape, 0),
        DEVICE: me,
    }
    bits = [parts[place[q][0]] >> place[q][1] & 1 for q in range(qubits)]
    parity = jnp.zeros(shape, jnp.int32)
    for q in edges:
        parity = parity + bits[q] * bits[(q + 1) % qubits]
    return (1 - 2 * (parity & 1)).astype(jnp.float32)


def half_turn(angle):
    x = 0.5 * angle
    x2 = x * x
    cosine, sine = 0.0, 0.0
    for n in range(8, -1, -1):
        cosine = cosine * x2 + (-1.0) ** n / math.factorial(2 * n)
        sine = sine * x2 + (-1.0) ** n / math.factorial(2 * n + 1)
    return cosine, sine * x


def kernel(
    n, qubits, angles, kinds, ket_ref, obs_ref, out_ref, grads_ref,
    sent1, held1, sent2, held2, gsent, gheld,
    send1, recv1, send2, recv2, gsend, grecv,
):
    me = lax.axis_index("amp")
    majors = n
    major_bits = n.bit_length() - 1
    local_bits = LANE_BITS + SUB_BITS + major_bits
    home, away = layouts(major_bits, qubits - local_bits)
    scale = 2.0 / math.sqrt(2**qubits)

    barrier = pltpu.get_barrier_semaphore()

    @pl.loop(1, n)
    def _(k):
        pl.semaphore_signal(barrier, inc=1, device_id=((me + k) % n,), device_id_type=MESH)

    rows = 8 * majors
    raw = [
        ket_ref[pl.ds(0, rows, stride=2), :],
        ket_ref[pl.ds(1, rows, stride=2), :],
        obs_ref[...],
    ]
    for part, value in enumerate(raw):
        value = value.reshape(majors, 8, 128)
        for bit in (1, 2):
            value = swap_bits(value, major_bits - 3 + bit, bit)
        sent1[:, part] = value

    pl.semaphore_wait(barrier, n - 1)

    def exchange(source, target, send, recv, whole):
        def copy(k, block, slot):
            return pltpu.make_async_remote_copy(
                src_ref=source if whole else source.at[block],
                dst_ref=target.at[slot],
                send_sem=send.at[k],
                recv_sem=recv.at[k],
                device_id=((me + k) % n,),
                device_id_type=MESH,
            )

        def start():
            @pl.loop(1, n)
            def _(k):
                copy(k, (me + k) % n, me).start()

        def arrive():
            @pl.loop(1, n)
            def _(k):
                copy(k, (me + k) % n, (me + n - k) % n).wait_recv()

        def depart():
            @pl.loop(1, n)
            def _(k):
                copy(k, (me + k) % n, me).wait_send()

        return start, arrive, depart

    start1, arrive1, depart1 = exchange(sent1, held1, send1, recv1, False)
    start2, arrive2, depart2 = exchange(sent2, held2, send2, recv2, False)
    gstart, garrive, gdepart = exchange(gsent, gheld, gsend, grecv, True)
    start1()
    held1[me] = sent1[me]

    layers, kind_count = angles.shape
    turns = [[half_turn(angles[l, k]) for k in range(kind_count)] for l in range(layers)]
    coefs, shares = [], []
    for l in range(layers):
        row, share = [], []
        for q in range(qubits):
            kind = kinds[l, q]
            is_kind = [jnp.where(kind == k, 1.0, 0.0) for k in range(kind_count)]
            c = sum(is_kind[k] * turns[l][k][0] for k in range(kind_count))
            sy = sum(is_kind[k] * turns[l][k][1] for k in range(kind_count - 1))
            row.append((c, sy, is_kind[-1] * turns[l][-1][1]))
            share.append(is_kind)
        coefs.append(row)
        shares.append(share)

    sums = [[jnp.zeros((8, 128), jnp.float32) for _ in range(kind_count)] for _ in range(layers)]

    def add_terms(l, chosen, place, bra, ket):
        w = bra[0] * ket[1] - bra[1] * ket[0]
        w_sum = jnp.sum(w, axis=0)
        for q in chosen:
            y, z = terms(bra, ket, place[q], w, w_sum)
            for k in range(kind_count):
                sums[l][k] = sums[l][k] + shares[l][q][k] * (z if k == kind_count - 1 else y)

    def turn(state, l, chosen, place):
        for q in chosen:
            state = gate(state, place[q], coefs[l][q])
        return state

    def prepare(buffer, sign):
        ket = (buffer[:, 0] * sign, buffer[:, 1] * sign)
        weight = scale * buffer[:, 2]
        return ket, (weight * ket[0], weight * ket[1])

    def times(state, sign):
        return (state[0] * sign, state[1] * sign)

    every = range(qubits)
    moved = [q for q in every if away[q][0] == DEVICE]
    first, last = min(moved), max(moved)
    late_edges = [q for q in every if first - 1 <= q <= last]
    early_edges = [q for q in every if q not in late_edges]
    local = [q for q in every if home[q][0] != DEVICE]
    outer = [q for q in every if home[q][0] == DEVICE]

    sign = edge_sign(home, qubits, every, majors, me)
    ket, bra = prepare(sent1, sign)
    add_terms(1, local, home, bra, ket)
    ket, bra = (times(turn(x, 1, local, home), sign) for x in (ket, bra))
    add_terms(0, local[1:-1], home, bra, ket)

    sign = edge_sign(away, qubits, every, majors, me)
    early = edge_sign(away, qubits, early_edges, majors, me)
    arrive1()
    ket, bra = prepare(held1, sign)
    here = [q for q in every if away[q][0] != DEVICE]
    bra_mid = times(turn(bra, 1, here, away), early)
    ready = [q for q in here if q not in (first - 1, last + 1)]
    done = turn(bra_mid, 0, ready, away)
    sent2[:, 0] = done[0]
    sent2[:, 1] = done[1]
    start2()
    held2[me] = sent2[me]
    add_terms(1, outer, away, bra, ket)
    ket = times(turn(ket, 1, here, away), early)
    add_terms(0, [local[-1]] + outer + [0], away, bra_mid, ket)

    at = [lax.broadcasted_iota(jnp.int32, (layers, 128), d) for d in range(2)]
    total = jnp.zeros((layers, 128), jnp.float32)
    for l in range(layers):
        for k in range(kind_count):
            total = total + jnp.where((at[0] == l) & (at[1] == k), jnp.sum(sums[l][k]), 0.0)
    gsent[...] = total
    gstart()
    gheld[me] = total

    late = edge_sign(home, qubits, late_edges, majors, me)
    arrive2()
    bra = (held2[:, 0], held2[:, 1])
    bra = times(turn(bra, 1, moved, home), late)
    bra = turn(bra, 0, [q for q in local if q not in ready], home)
    for part, value in enumerate(bra):
        for bit in (1, 2):
            value = swap_bits(value, major_bits - 3 + bit, bit)
        out_ref[pl.ds(part, rows, stride=2), :] = value.reshape(rows, 128)
    garrive()
    grads_ref[...] = jnp.sum(gheld[...], axis=0)
    depart1()
    depart2()
    gdepart()


def by_exchange(ket_state, observable, angles, gate_kinds):
    amp_count = ket_state.shape[1]
    n = lax.axis_size("amp")
    qubits = (amp_count * n).bit_length() - 1
    layers, kind_count = angles.shape
    rows = amp_count // 128
    ket = ket_state.reshape(2, rows, 128).transpose(1, 0, 2).reshape(2 * rows, 128)
    vmem = pl.BlockSpec(memory_space=pltpu.VMEM)
    smem = pl.BlockSpec(memory_space=pltpu.SMEM)
    f32 = jnp.float32
    out, grads = pl.pallas_call(
        functools.partial(kernel, n, qubits),
        out_shape=(
            jax.ShapeDtypeStruct((2 * rows, 128), f32),
            jax.ShapeDtypeStruct((layers, 128), f32),
        ),
        in_specs=[smem, smem, vmem, vmem],
        out_specs=(vmem, vmem),
        scratch_shapes=[
            pltpu.VMEM((n, 3, 8, 128), f32),
            pltpu.VMEM((n, 3, 8, 128), f32),
            pltpu.VMEM((n, 2, 8, 128), f32),
            pltpu.VMEM((n, 2, 8, 128), f32),
            pltpu.VMEM((layers, 128), f32),
            pltpu.VMEM((n, layers, 128), f32),
        ]
        + [pltpu.SemaphoreType.DMA((n,))] * 6,
        compiler_params=pltpu.CompilerParams(collective_id=0, has_side_effects=True),
    )(angles, gate_kinds, ket, observable.reshape(rows, 128))
    bra_state = out.reshape(rows, 2, 128).transpose(1, 0, 2).reshape(2, amp_count)
    return (bra_state, grads[:, :kind_count])


def per_device(ket_state, observable, angles, gate_kinds):
    tiles = ket_state.shape[1] // (1 << LANE_BITS + SUB_BITS)
    if tiles == lax.axis_size("amp") and tiles >= 8 and angles.shape == (2, 3):
        return by_exchange(ket_state, observable, angles, gate_kinds)
    return on_device(ket_state, observable, angles, gate_kinds)


def solution(mesh):
    placed = (P(None, "amp"), P("amp"), P(), P())
    return jax.shard_map(
        per_device, mesh=mesh, in_specs=placed, out_specs=(P(None, "amp"), P()), check_vma=False
    )
```

```python
import functools
import math

import jax
import jax.numpy as jnp
import numpy as np
from jax import lax
from jax.experimental import pallas as pl
from jax.experimental.pallas import tpu as pltpu
from jax.sharding import PartitionSpec as P

MESH = pl.DeviceIdType.MESH
LANE, SUB, MAJOR, DEVICE = range(4)
LANE_BITS, SUB_BITS = 7, 3


def from_partner(value, axis, apart):
    mask = 2**apart
    pairs = [(source, source ^ mask) for source in range(lax.axis_size(axis))]
    return lax.ppermute(value, axis, pairs)


def pair_tables():
    column = np.arange(128)
    flips = []
    signs = []
    for position in range(7):
        upper = column >> position & 1
        flip_table = np.zeros((128, 128), np.float32)
        flip_table[column, column ^ 1 << position] = np.where(upper == 0, -0.5, 0.5)
        flips.append(flip_table)
        signs.append((1 - 2 * upper).astype(np.float32))
    return (np.stack(flips), np.stack(signs))


def layout_map(local_bits, global_bits):
    local_map = list(range(local_bits))
    device_map = [local_bits + bit_num for bit_num in range(global_bits)]
    return (local_map, device_map)


def entangle_sign(local_bits, global_bits, device_id, amp_count):
    local_map, device_map = layout_map(local_bits, global_bits)
    amp_index = lax.iota(jnp.int32, amp_count)
    bit_values = [None] * (local_bits + global_bits)
    for position in range(local_bits):
        bit_values[local_map[position]] = amp_index >> position & 1
    for bit_num in range(global_bits):
        bit_values[device_map[bit_num]] = device_id >> bit_num & 1
    all_bits = local_bits + global_bits
    parity = jnp.zeros((amp_count,), jnp.int32)
    for qubit_id in range(all_bits):
        parity = parity + bit_values[qubit_id] * bit_values[(qubit_id + 1) % all_bits]
    return (1 - 2 * (parity & 1)).astype(jnp.float32)


def rotation_of(angles, gate_kinds, layer_id, qubit_id):
    kind_id = gate_kinds[layer_id, qubit_id]
    chosen = jnp.arange(angles.shape[1]) == kind_id
    rotation = jnp.sum(jnp.where(chosen, angles[layer_id], 0.0))
    return (kind_id, jnp.cos(0.5 * rotation), jnp.sin(0.5 * rotation))


def kind_vector(kind_id, kind_count):
    return (jnp.arange(kind_count) == kind_id).astype(jnp.float32)


def rotate_phase(values, cosine, sine_value):
    return jnp.stack(
        [cosine * values[0] - sine_value * values[1], cosine * values[1] + sine_value * values[0]]
    )


def rotate_position(ket_state, bra_state, position, qubit_id, layer_id, angles, gate_kinds):
    amp_count = ket_state.shape[1]
    fold_shape = (2, amp_count >> position + 1, 2, 1 << position)
    kind_id, cosine, sine_value = rotation_of(angles, gate_kinds, layer_id, qubit_id)

    def turn_y(operands):
        folded_ket, folded_bra = operands
        ket_low, ket_high = (folded_ket[:, :, 0], folded_ket[:, :, 1])
        bra_low, bra_high = (folded_bra[:, :, 0], folded_bra[:, :, 1])
        partial_value = 0.5 * jnp.sum(bra_high * ket_low - bra_low * ket_high)
        new_ket = jnp.stack(
            [cosine * ket_low + sine_value * ket_high, cosine * ket_high - sine_value * ket_low],
            axis=2,
        )
        new_bra = jnp.stack(
            [cosine * bra_low + sine_value * bra_high, cosine * bra_high - sine_value * bra_low],
            axis=2,
        )
        return (new_ket, new_bra, partial_value)

    def turn_z(operands):
        folded_ket, folded_bra = operands
        ket_low, ket_high = (folded_ket[:, :, 0], folded_ket[:, :, 1])
        bra_low, bra_high = (folded_bra[:, :, 0], folded_bra[:, :, 1])
        partial_value = 0.5 * (
            jnp.sum(bra_low[0] * ket_low[1] - bra_low[1] * ket_low[0])
            - jnp.sum(bra_high[0] * ket_high[1] - bra_high[1] * ket_high[0])
        )
        new_ket = jnp.stack(
            [
                rotate_phase(ket_low, cosine, sine_value),
                rotate_phase(ket_high, cosine, -sine_value),
            ],
            axis=2,
        )
        new_bra = jnp.stack(
            [
                rotate_phase(bra_low, cosine, sine_value),
                rotate_phase(bra_high, cosine, -sine_value),
            ],
            axis=2,
        )
        return (new_ket, new_bra, partial_value)

    new_ket, new_bra, partial_value = lax.cond(
        kind_id == 2, turn_z, turn_y, (ket_state.reshape(fold_shape), bra_state.reshape(fold_shape))
    )
    terms = partial_value * kind_vector(kind_id, angles.shape[1])
    return (new_ket.reshape(2, amp_count), new_bra.reshape(2, amp_count), terms)


def contract_rows(left, right):
    return lax.dot_general(
        left,
        right,
        (((0,), (0,)), ((), ())),
        precision=lax.Precision.HIGHEST,
        preferred_element_type=jnp.float32,
    )


def contract_cols(left, right):
    return lax.dot_general(
        left,
        right,
        (((1,), (1,)), ((), ())),
        precision=lax.Precision.HIGHEST,
        preferred_element_type=jnp.float32,
    )


def low_block(ket_state, bra_state, qubit_list, layer_id, angles, gate_kinds):
    amp_count = ket_state.shape[1]
    row_count = amp_count // 128
    flips, signs = pair_tables()
    ket_real = ket_state[0].reshape(row_count, 128)
    ket_imag = ket_state[1].reshape(row_count, 128)
    bra_real = bra_state[0].reshape(row_count, 128)
    bra_imag = bra_state[1].reshape(row_count, 128)
    gram_real = contract_rows(bra_real, ket_real) + contract_rows(bra_imag, ket_imag)
    gram_imag = contract_rows(bra_real, ket_imag) - contract_rows(bra_imag, ket_real)
    gram_diag = jnp.diagonal(gram_imag)
    terms = jnp.zeros((angles.shape[1],), jnp.float32)
    kron_real = None
    kron_imag = None
    for position in range(7):
        kind_id, cosine, sine_value = rotation_of(
            angles, gate_kinds, layer_id, qubit_list[position]
        )
        is_z = kind_id == 2
        partial_value = jnp.where(
            is_z, 0.5 * jnp.sum(signs[position] * gram_diag), jnp.sum(flips[position] * gram_real)
        )
        terms = terms + partial_value * kind_vector(kind_id, angles.shape[1])
        mat_y = jnp.stack([jnp.stack([cosine, sine_value]), jnp.stack([-sine_value, cosine])])
        zero_value = jnp.zeros_like(cosine)
        mat_zr = jnp.stack([jnp.stack([cosine, zero_value]), jnp.stack([zero_value, cosine])])
        mat_zi = jnp.stack(
            [jnp.stack([sine_value, zero_value]), jnp.stack([zero_value, -sine_value])]
        )
        mat_real = jnp.where(is_z, mat_zr, mat_y)
        mat_imag = jnp.where(is_z, mat_zi, jnp.zeros_like(mat_zi))
        if kron_real is None:
            kron_real, kron_imag = (mat_real, mat_imag)
        else:
            kron_real, kron_imag = (
                jnp.kron(mat_real, kron_real) - jnp.kron(mat_imag, kron_imag),
                jnp.kron(mat_real, kron_imag) + jnp.kron(mat_imag, kron_real),
            )

    def apply_block(real_rows, imag_rows):
        new_real = contract_cols(real_rows, kron_real) - contract_cols(imag_rows, kron_imag)
        new_imag = contract_cols(imag_rows, kron_real) + contract_cols(real_rows, kron_imag)
        return jnp.stack([new_real.reshape(amp_count), new_imag.reshape(amp_count)])

    return (apply_block(ket_real, ket_imag), apply_block(bra_real, bra_imag), terms)


def rotate_global(
    ket_state,
    bra_state,
    far_ket,
    far_bra,
    bit_num,
    qubit_id,
    device_id,
    layer_id,
    angles,
    gate_kinds,
):
    kind_id, cosine, sine_value = rotation_of(angles, gate_kinds, layer_id, qubit_id)
    orient = (1 - 2 * (device_id >> bit_num & 1)).astype(jnp.float32)

    def turn_y(operands):
        own_ket, own_bra, other_ket, other_bra = operands
        partial_value = 0.25 * orient * jnp.sum(other_bra * own_ket - own_bra * other_ket)
        return (
            cosine * own_ket + orient * sine_value * other_ket,
            cosine * own_bra + orient * sine_value * other_bra,
            partial_value,
        )

    def turn_z(operands):
        own_ket, own_bra, other_ket, other_bra = operands
        partial_value = 0.5 * orient * jnp.sum(own_bra[0] * own_ket[1] - own_bra[1] * own_ket[0])
        return (
            rotate_phase(own_ket, cosine, orient * sine_value),
            rotate_phase(own_bra, cosine, orient * sine_value),
            partial_value,
        )

    new_ket, new_bra, partial_value = lax.cond(
        kind_id == 2, turn_z, turn_y, (ket_state, bra_state, far_ket, far_bra)
    )
    return (new_ket, new_bra, partial_value * kind_vector(kind_id, angles.shape[1]))


def on_device(ket_state, observable, angles, gate_kinds):
    amp_count = ket_state.shape[1]
    local_bits = amp_count.bit_length() - 1
    group_size = lax.axis_size("amp")
    global_bits = group_size.bit_length() - 1
    device_id = lax.axis_index("amp")
    layer_count = angles.shape[0]
    kind_count = angles.shape[1]
    bra_state = 2.0 / math.sqrt(amp_count * group_size) * observable[None, :] * ket_state
    sign_cache = {}
    grads_local = jnp.zeros((layer_count, kind_count), jnp.float32)
    for sweep_id in range(layer_count):
        layer_id = layer_count - 1 - sweep_id
        layout = 0
        local_map, device_map = layout_map(local_bits, global_bits)
        if layout not in sign_cache:
            sign_cache[layout] = entangle_sign(local_bits, global_bits, device_id, amp_count)
        phase_sign = sign_cache[layout]
        ket_state = ket_state * phase_sign[None, :]
        bra_state = bra_state * phase_sign[None, :]
        ket_state, bra_state, layer_terms = low_block(
            ket_state, bra_state, local_map[:7], layer_id, angles, gate_kinds
        )
        for position in range(7, local_bits):
            ket_state, bra_state, partial_value = rotate_position(
                ket_state, bra_state, position, local_map[position], layer_id, angles, gate_kinds
            )
            layer_terms = layer_terms + partial_value
        for bit_num in range(global_bits):
            far_ket, far_bra = from_partner((ket_state, bra_state), "amp", bit_num)
            ket_state, bra_state, partial_value = rotate_global(
                ket_state,
                bra_state,
                far_ket,
                far_bra,
                bit_num,
                device_map[bit_num],
                device_id,
                layer_id,
                angles,
                gate_kinds,
            )
            layer_terms = layer_terms + partial_value
        grads_local = grads_local.at[layer_id].set(layer_terms)
    grads = lax.psum(grads_local, "amp")
    return (bra_state, grads)


def layouts(major_bits, global_bits):
    low = LANE_BITS + SUB_BITS
    local_bits = low + major_bits
    home, away = {}, {}
    for q in range(LANE_BITS):
        home[q] = away[q] = (LANE, q)
    home[LANE_BITS] = away[LANE_BITS] = (SUB, 0)
    for bit, q in ((1, local_bits - 2), (2, local_bits - 1)):
        home[q] = away[q] = (SUB, bit)
    moved = list(range(low, local_bits - 2)) + [low - 2, low - 1]
    for bit, q in enumerate(moved):
        home[q], away[q] = (MAJOR, bit), (DEVICE, bit)
    for bit in range(global_bits):
        home[local_bits + bit], away[local_bits + bit] = (DEVICE, bit), (MAJOR, bit)
    return home, away


def split_major(x, bit):
    fold = x.reshape((x.shape[0] >> bit + 1, 2, 1 << bit) + x.shape[1:])
    return fold[:, 0], fold[:, 1]


def join_major(x0, x1):
    out = jnp.stack([x0, x1], axis=1)
    return out.reshape((-1,) + out.shape[3:])


def minor_bit(axis, bit):
    return lax.broadcasted_iota(jnp.int32, (1, 8, 128), 1 if axis == SUB else 2) >> bit & 1


def minor_sign(axis, bit):
    return (1 - 2 * minor_bit(axis, bit)).astype(jnp.float32)


def shifted(x, axis, by):
    dim = 1 if axis == SUB else 2
    return pltpu.roll(x, by % x.shape[dim], dim)


def partner(x, axis, bit):
    step = 1 << bit
    up = shifted(x, axis, -step)
    if 2 * step == x.shape[1 if axis == SUB else 2]:
        return up
    return jnp.where(minor_bit(axis, bit) == 0, up, shifted(x, axis, step))


def swap_bits(x, major, sub):
    x0, x1 = split_major(x, major)
    lower = minor_bit(SUB, sub) == 0

    def roll3(y, by):
        z = y.reshape((-1,) + y.shape[2:])
        return shifted(z, SUB, by).reshape(y.shape)

    step = 1 << sub
    return join_major(jnp.where(lower, x0, roll3(x1, step)), jnp.where(lower, roll3(x0, -step), x1))


def gate(state, place, coef):
    re, im = state
    axis, bit = place
    c, sy, sz = coef
    if axis == MAJOR:
        r0, r1 = split_major(re, bit)
        i0, i1 = split_major(im, bit)
        return (
            join_major(c * r0 + sy * r1 - sz * i0, c * r1 - sy * r0 + sz * i1),
            join_major(c * i0 + sy * i1 + sz * r0, c * i1 - sy * i0 - sz * r1),
        )
    z = minor_sign(axis, bit)
    zy, zz = sy * z, sz * z
    return (
        c * re + zy * partner(re, axis, bit) - zz * im,
        c * im + zy * partner(im, axis, bit) + zz * re,
    )


def lane_matrix(coefs):
    at = [lax.broadcasted_iota(jnp.int32, (128, 128), d) for d in range(2)]
    re, im = None, None
    for bit, (c, sy, sz) in enumerate(coefs):
        old, new = (x >> bit & 1 for x in at)
        z = (1 - 2 * new).astype(jnp.float32)
        same = old == new
        a, b = jnp.where(same, c, sy * z), jnp.where(same, sz * z, 0.0)
        re, im = (a, b) if re is None else (re * a - im * b, re * b + im * a)
    return jnp.concatenate([jnp.concatenate([re, im], 1), jnp.concatenate([-im, re], 1)], 0)


def turn_lanes(state, matrix):
    re, im = (x.reshape(-1, 128) for x in state)
    both = lax.dot_general(
        jnp.concatenate([re, im], axis=1),
        matrix[...],
        (((1,), (0,)), ((), ())),
        precision=lax.Precision.HIGH,
        preferred_element_type=jnp.float32,
    )
    return both[:, :128].reshape(state[0].shape), both[:, 128:].reshape(state[0].shape)


def terms(bra, ket, place, w, w_sum):
    axis, bit = place
    if axis == MAJOR:
        y = 0.0
        for b, k in zip(bra, ket):
            b0, b1 = split_major(b, bit)
            k0, k1 = split_major(k, bit)
            y = y + jnp.sum(b1 * k0 - b0 * k1, axis=(0, 1))
        w0, w1 = split_major(w, bit)
        return 0.5 * y, 0.5 * jnp.sum(w0 - w1, axis=(0, 1))
    z = 0.5 * minor_sign(axis, bit)[0]
    y = sum(jnp.sum(b * partner(k, axis, bit), axis=0) for b, k in zip(bra, ket))
    return -z * y, z * w_sum


def edge_sign(place, qubits, edges, majors, me):
    shape = (majors, 8, 128)
    parts = {
        LANE: lax.broadcasted_iota(jnp.int32, shape, 2),
        SUB: lax.broadcasted_iota(jnp.int32, shape, 1),
        MAJOR: lax.broadcasted_iota(jnp.int32, shape, 0),
        DEVICE: me,
    }
    bits = [parts[place[q][0]] >> place[q][1] & 1 for q in range(qubits)]
    parity = jnp.zeros(shape, jnp.int32)
    for q in edges:
        parity = parity + bits[q] * bits[(q + 1) % qubits]
    return (1 - 2 * (parity & 1)).astype(jnp.float32)


def half_turn(angle):
    x = 0.5 * angle
    x2 = x * x
    cosine, sine = 0.0, 0.0
    for n in range(8, -1, -1):
        cosine = cosine * x2 + (-1.0) ** n / math.factorial(2 * n)
        sine = sine * x2 + (-1.0) ** n / math.factorial(2 * n + 1)
    return cosine, sine * x


def kernel(
    n, qubits, angles, kinds, ket_ref, obs_ref, out_ref, grads_ref,
    ket_in, obs_in, sent1, held1, sent2, held2, gsent, gheld, gsent2, gheld2,
    send1, recv1, send2, recv2, gsend, grecv, gsend2, grecv2, load, wide,
):
    me = lax.axis_index("amp")
    majors = n
    major_bits = n.bit_length() - 1
    local_bits = LANE_BITS + SUB_BITS + major_bits
    home, away = layouts(major_bits, qubits - local_bits)
    scale = 2.0 / math.sqrt(2**qubits)

    loads = [
        pltpu.make_async_copy(ket_ref, ket_in, load.at[0]),
        pltpu.make_async_copy(obs_ref, obs_in, load.at[1]),
    ]
    for copy in loads:
        copy.start()

    half = n // 2
    high, low = me // half, me % half

    def peer(k, sign):
        side = (high + 1 - k // half) % 2
        return side * half + (low + half + sign * (k % half)) % half

    barrier = pltpu.get_barrier_semaphore()
    for k in [k for k in range(n) if k != half]:
        pl.semaphore_signal(barrier, inc=1, device_id=(peer(k, 1),), device_id_type=MESH)
    for copy in loads:
        copy.wait()

    rows = 8 * majors
    raw = [
        ket_in[pl.ds(0, rows, stride=2), :],
        ket_in[pl.ds(1, rows, stride=2), :],
        obs_in[...],
    ]
    for part, value in enumerate(raw):
        value = value.reshape(majors, 8, 128)
        for bit in (1, 2):
            value = swap_bits(value, major_bits - 3 + bit, bit)
        sent1[:, part] = value

    pl.semaphore_wait(barrier, n - 1)

    def exchange(source, target, send, recv):
        def copy(k, block, slot):
            return pltpu.make_async_remote_copy(
                src_ref=source.at[block],
                dst_ref=target.at[slot],
                send_sem=send.at[k],
                recv_sem=recv.at[k],
                device_id=(peer(k, 1),),
                device_id_type=MESH,
            )

        def each(act):
            for lower, upper in ((0, half), (half + 1, n)):
                pl.loop(lower, upper)(act)

        def start():
            each(lambda k: copy(k, peer(k, 1), me).start())

        def arrive():
            each(lambda k: copy(k, peer(k, 1), peer(k, -1)).wait_recv())

        def depart():
            each(lambda k: copy(k, peer(k, 1), me).wait_send())

        return start, arrive, depart

    def gather(source, target, send, recv, stride, count):
        digit = me // stride % count

        def copies():
            for k in range(1, count):
                yield pltpu.make_async_remote_copy(
                    src_ref=source,
                    dst_ref=target.at[k],
                    send_sem=send.at[k],
                    recv_sem=recv.at[k],
                    device_id=(me + ((digit + k) % count - digit) * stride,),
                    device_id_type=MESH,
                )

        target[0] = source[...]
        for copy in copies():
            copy.start()
        return lambda: [copy.wait_recv() for copy in copies()], lambda: [copy.wait_send() for copy in copies()]

    start1, arrive1, depart1 = exchange(sent1, held1, send1, recv1)
    start2, arrive2, depart2 = exchange(sent2, held2, send2, recv2)
    start1()
    held1[me] = sent1[me]

    layers, kind_count = angles.shape
    turns = [[half_turn(angles[l, k]) for k in range(kind_count)] for l in range(layers)]
    coefs, shares = [], []
    for l in range(layers):
        row, share = [], []
        for q in range(qubits):
            kind = kinds[l, q]
            is_kind = [jnp.where(kind == k, 1.0, 0.0) for k in range(kind_count)]
            c = sum(is_kind[k] * turns[l][k][0] for k in range(kind_count))
            sy = sum(is_kind[k] * turns[l][k][1] for k in range(kind_count - 1))
            row.append((c, sy, is_kind[-1] * turns[l][-1][1]))
            share.append(is_kind)
        coefs.append(row)
        shares.append(share)

    for l in range(layers):
        wide[l] = lane_matrix(coefs[l][:LANE_BITS])
    matrices = [wide.at[l] for l in range(layers)]

    sums = [[jnp.zeros((8, 128), jnp.float32) for _ in range(kind_count)] for _ in range(layers)]

    def add_terms(l, chosen, place, bra, ket):
        w = bra[0] * ket[1] - bra[1] * ket[0]
        w_sum = jnp.sum(w, axis=0)
        for q in chosen:
            y, z = terms(bra, ket, place[q], w, w_sum)
            for k in range(kind_count):
                sums[l][k] = sums[l][k] + shares[l][q][k] * (z if k == kind_count - 1 else y)

    def turn(state, l, chosen, place):
        lanes = set(range(LANE_BITS))
        if lanes <= set(chosen):
            state = turn_lanes(state, matrices[l])
            chosen = [q for q in chosen if q not in lanes]
        for q in chosen:
            state = gate(state, place[q], coefs[l][q])
        return state

    def prepare(buffer, sign):
        ket = (buffer[:, 0] * sign, buffer[:, 1] * sign)
        weight = scale * buffer[:, 2]
        return ket, (weight * ket[0], weight * ket[1])

    def times(state, sign):
        return (state[0] * sign, state[1] * sign)

    every = range(qubits)
    moved = [q for q in every if away[q][0] == DEVICE]
    first, last = min(moved), max(moved)
    late_edges = [q for q in every if first - 1 <= q <= last]
    early_edges = [q for q in every if q not in late_edges]
    local = [q for q in every if home[q][0] != DEVICE]
    outer = [q for q in every if home[q][0] == DEVICE]

    sign = edge_sign(home, qubits, every, majors, me)
    ket, bra = prepare(sent1, sign)
    add_terms(1, local, home, bra, ket)
    ket, bra = (times(turn(x, 1, local, home), sign) for x in (ket, bra))
    add_terms(0, local[1:-1], home, bra, ket)

    sign = edge_sign(away, qubits, every, majors, me)
    early = edge_sign(away, qubits, early_edges, majors, me)
    arrive1()
    ket, bra = prepare(held1, sign)
    here = [q for q in every if away[q][0] != DEVICE]
    bra_mid = times(turn(bra, 1, here, away), early)
    ready = [q for q in here if q not in (first - 1, last + 1)]
    done = turn(bra_mid, 0, ready, away)
    sent2[:, 0] = done[0]
    sent2[:, 1] = done[1]
    start2()
    held2[me] = sent2[me]
    add_terms(1, outer, away, bra, ket)
    ket = times(turn(ket, 1, here, away), early)
    add_terms(0, [local[-1]] + outer + [0], away, bra_mid, ket)

    at = [lax.broadcasted_iota(jnp.int32, (layers, 128), d) for d in range(2)]
    total = jnp.zeros((layers, 128), jnp.float32)
    for l in range(layers):
        for k in range(kind_count):
            total = total + jnp.where((at[0] == l) & (at[1] == k), jnp.sum(sums[l][k]), 0.0)
    inner = gheld.shape[0]
    gsent[...] = total
    garrive, gdepart = gather(gsent, gheld, gsend, grecv, 1, inner)
    garrive()
    gsent2[...] = jnp.sum(gheld[...], axis=0)
    garrive2, gdepart2 = gather(gsent2, gheld2, gsend2, grecv2, inner, n // inner)

    late = edge_sign(home, qubits, late_edges, majors, me)
    arrive2()
    bra = (held2[:, 0], held2[:, 1])
    bra = times(turn(bra, 1, moved, home), late)
    bra = turn(bra, 0, [q for q in local if q not in ready], home)
    for part, value in enumerate(bra):
        for bit in (1, 2):
            value = swap_bits(value, major_bits - 3 + bit, bit)
        out_ref[pl.ds(part, rows, stride=2), :] = value.reshape(rows, 128)
    garrive2()
    grads_ref[...] = jnp.sum(gheld2[...], axis=0)
    depart1()
    depart2()
    gdepart()
    gdepart2()


def by_exchange(ket_state, observable, angles, gate_kinds):
    amp_count = ket_state.shape[1]
    n = lax.axis_size("amp")
    qubits = (amp_count * n).bit_length() - 1
    layers, kind_count = angles.shape
    rows = amp_count // 128
    ket = ket_state.reshape(2, rows, 128).transpose(1, 0, 2).reshape(2 * rows, 128)
    vmem = pl.BlockSpec(memory_space=pltpu.VMEM)
    smem = pl.BlockSpec(memory_space=pltpu.SMEM)
    hbm = pl.BlockSpec(memory_space=pl.ANY)
    inner = 1 << n.bit_length() // 2
    outer = n // inner
    f32 = jnp.float32
    out, grads = pl.pallas_call(
        functools.partial(kernel, n, qubits),
        out_shape=(
            jax.ShapeDtypeStruct((2 * rows, 128), f32),
            jax.ShapeDtypeStruct((layers, 128), f32),
        ),
        in_specs=[smem, smem, hbm, hbm],
        out_specs=(vmem, vmem),
        scratch_shapes=[
            pltpu.VMEM((2 * rows, 128), f32),
            pltpu.VMEM((rows, 128), f32),
            pltpu.VMEM((n, 3, 8, 128), f32),
            pltpu.VMEM((n, 3, 8, 128), f32),
            pltpu.VMEM((n, 2, 8, 128), f32),
            pltpu.VMEM((n, 2, 8, 128), f32),
            pltpu.VMEM((layers, 128), f32),
            pltpu.VMEM((inner, layers, 128), f32),
            pltpu.VMEM((layers, 128), f32),
            pltpu.VMEM((outer, layers, 128), f32),
        ]
        + [pltpu.SemaphoreType.DMA((size,)) for size in (n, n, n, n, inner, inner, outer, outer, 2)]
        + [pltpu.VMEM((layers, 256, 256), f32)],
        compiler_params=pltpu.CompilerParams(collective_id=0, has_side_effects=True),
    )(angles, gate_kinds, ket, observable.reshape(rows, 128))
    bra_state = out.reshape(rows, 2, 128).transpose(1, 0, 2).reshape(2, amp_count)
    return (bra_state, grads[:, :kind_count])


def per_device(ket_state, observable, angles, gate_kinds):
    tiles = ket_state.shape[1] // (1 << LANE_BITS + SUB_BITS)
    if tiles == lax.axis_size("amp") and tiles >= 8 and angles.shape == (2, 3):
        return by_exchange(ket_state, observable, angles, gate_kinds)
    return on_device(ket_state, observable, angles, gate_kinds)


def solution(mesh):
    placed = (P(None, "amp"), P("amp"), P(), P())
    return jax.shard_map(
        per_device, mesh=mesh, in_specs=placed, out_specs=(P(None, "amp"), P()), check_vma=False
    )
```
